32 devices in a mesh: batch: 4 (over y, x), proto: 8 (over z, core).
Axes of the slice: x: 2, y: 2, z: 4, core: 2. Of those that a mesh axis runs over, the one named last changes fastest.
Arguments:
- view_codes: bfloat16 [4096, 1024], P('batch', 'proto'), may hold values from -80 to 80
- predictor_view_embeddings: bfloat16 [4096, 1024], P('batch', 'proto'), may hold values from -80 to 80
- prototypes: bfloat16 [65536, 1024], P('proto'), may hold values from -64 to 64
Outputs:
- assignments: bfloat16 [4096, 65536], P('batch', 'proto')
- loss_rows: float32 [4096], P('batch')
The draws below stay inside these ranges and needn't reach their ends.
All inputs are finite; a program needn't handle non-finite values.
Results may differ from the reference program's by a relative error of at most 0.0034.
Values may be sent and summed in bfloat16 or wider, within the bound.
No kernel may reach another device: no remote copies, remote signals or barrier semaphores. Data moves between devices by JAX's collectives and lax.ppermute only.
A program may use at most 128 MiB of HBM per device.

```python
import jax
import jax.numpy as jnp
from jax import lax

D = 1024
PROTOS = 65536
SINK_ITERS = 3
BATCH = 4096


def shared_centres(key):
    base_key = jax.random.fold_in(key, 17)
    keys = jax.random.split(base_key, 3)
    groups = PROTOS // 16
    centres = jax.random.truncated_normal(keys[0], -3.0, 3.0, (groups, D), jnp.float32)
    labels = jax.random.randint(keys[1], (BATCH,), 0, groups)
    owners = jax.random.randint(keys[2], (PROTOS,), 0, groups)
    return (centres, labels, owners)


def shared_views(key):
    centres, labels, owners = shared_centres(key)
    keys = jax.random.split(jax.random.fold_in(key, 29), 6)
    chosen = centres[labels]
    noise_first = jax.random.truncated_normal(keys[2], -4.0, 4.0, (BATCH, D), jnp.float32)
    noise_second = jax.random.truncated_normal(keys[3], -4.0, 4.0, (BATCH, D), jnp.float32)
    scale_first = jnp.exp(jax.random.uniform(keys[4], (BATCH, 1), jnp.float32, 0.0, 2.3))
    scale_second = jnp.exp(jax.random.uniform(keys[5], (BATCH, 1), jnp.float32, 0.0, 2.3))
    first = (chosen + 0.6 * noise_first) * scale_first
    second = (chosen + 0.6 * noise_second) * scale_second
    return (first, second)


def draw_view_codes(key, part):
    return shared_views(key)[0].astype(jnp.bfloat16)


def draw_predictor_view_embeddings(key, part):
    return shared_views(key)[1].astype(jnp.bfloat16)


def draw_prototypes(key, part):
    centres, labels, owners = shared_centres(key)
    keys = jax.random.split(jax.random.fold_in(key, 31), 2)
    chosen = centres[owners]
    noise = jax.random.truncated_normal(keys[0], -4.0, 4.0, (PROTOS, D), jnp.float32)
    scale = jnp.exp(jax.random.uniform(keys[1], (PROTOS, 1), jnp.float32, 0.0, 2.3))
    return ((chosen + 0.6 * noise) * scale).astype(jnp.bfloat16)


def setup_inputs(seed: int = 0) -> dict:
    streams_of = jax.random.split(jax.random.key(seed), 4)
    return {
        "view_codes": draw_view_codes(jax.random.fold_in(streams_of[3], 71), 0),
        "predictor_view_embeddings": draw_predictor_view_embeddings(jax.random.fold_in(streams_of[3], 71), 0),
        "prototypes": draw_prototypes(jax.random.fold_in(streams_of[3], 71), 0),
    }


EPSILON = 0.05
SOFTMAX_TEMP_VALUE = 0.1

def unit_protos(prototypes):
    weights = prototypes.astype(jnp.float32)
    return (weights * lax.rsqrt(lax.optimization_barrier(jnp.sum(weights * weights, axis=1, keepdims=True)) + 1e-06)).astype(jnp.bfloat16)

def tempered_scores(view, unit_prototype_rows):
    products = jnp.dot(view, unit_prototype_rows.T, preferred_element_type=jnp.float32)
    values = view.astype(jnp.float32)
    inverse_factor = lax.rsqrt(lax.optimization_barrier(jnp.sum(values * values, axis=1)) + 1e-06)
    return products * inverse_factor[:, None]

def reference(view_codes, predictor_view_embeddings, prototypes):
    unit_prototype_rows = unit_protos(prototypes)
    kernel = jnp.exp(tempered_scores(view_codes, unit_prototype_rows) / EPSILON)
    total_rows = kernel.shape[0]
    total_protos = kernel.shape[1]
    scale_rows = jnp.ones((total_rows,), jnp.float32)
    for iteration in range(SINK_ITERS):
        col_sums = jnp.dot(scale_rows, kernel, precision=lax.Precision.HIGHEST)
        scale_cols = 1.0 / (total_protos * col_sums)
        row_sums = jnp.dot(kernel, scale_cols, precision=lax.Precision.HIGHEST)
        scale_rows = 1.0 / (total_rows * row_sums)
    assign = kernel * scale_cols[None, :] * (total_rows * scale_rows)[:, None]
    assignments = (total_protos * assign).astype(jnp.bfloat16)
    logit_scores = tempered_scores(predictor_view_embeddings, unit_prototype_rows) / SOFTMAX_TEMP_VALUE
    totals = lax.optimization_barrier(jnp.sum(jnp.exp(logit_scores), axis=1))
    cross_term = lax.optimization_barrier(jnp.sum(assign * logit_scores, axis=1))
    loss_rows = jnp.log(totals) - cross_term
    return (assignments, loss_rows)
```

```python
import functools

import jax
import jax.numpy as jnp
from jax import lax
from jax.experimental import pallas as pl
from jax.experimental.pallas import tpu as pltpu
from jax.sharding import PartitionSpec as P

SINK_ITERS = 3
EPSILON = 0.05
SOFTMAX_TEMP_VALUE = 0.1
NORM_EPS = 1e-06
CHUNKS = 4
HALVES = 4
PIECES = 8
LANES = 128
LOGIT_STEPS = 3200.0


F32 = jnp.float32
BF16 = jnp.bfloat16
VM = pl.BlockSpec(memory_space=pltpu.VMEM)
HB = pl.BlockSpec(memory_space=pltpu.HBM)


def call(kernel, outs, ins, args, scratch=(), limit=6, flops=0, alias=None, name=None):
    big = lambda a: a.size * a.dtype.itemsize > (4 << 20)
    args = [
        pltpu.with_memory_space_constraint(a, pltpu.HBM if spec is HB else pltpu.VMEM) if spec is HB or big(a) else a
        for a, spec in zip(args, ins)
    ]
    return pl.pallas_call(
        kernel,
        out_shape=outs,
        in_specs=ins,
        out_specs=jax.tree.map(
            lambda o: HB if getattr(o, "memory_space", None) == pltpu.HBM else VM, outs
        ),
        scratch_shapes=list(scratch),
        input_output_aliases=alias or {},
        compiler_params=pltpu.CompilerParams(vmem_limit_bytes=limit << 20),
        cost_estimate=pl.CostEstimate(flops=int(flops), bytes_accessed=0, transcendentals=0),
        name=name,
    )(*args)


def rows_to_lanes(block):
    out = []
    for i in range(block.shape[0] // LANES):
        part = block[i * LANES : (i + 1) * LANES, :]
        out.append(jnp.sum(part.T, axis=0, keepdims=True))
    return jnp.concatenate(out, axis=0)


def lanes_to_rows(packed, out_ref):
    for i in range(packed.shape[0]):
        row = jnp.broadcast_to(packed[i : i + 1, :], (LANES, LANES))
        out_ref[i * LANES : (i + 1) * LANES, :] = row.T


def fetch(src, buf, sems, tile, i, slot, chunk=None):
    rows = pl.ds(pl.multiple_of(i * tile, tile), tile)
    if chunk is None:
        at = src.at[:, rows, :] if len(src.shape) == 3 else src.at[rows, :]
    else:
        at = src.at[chunk, rows, :]
    return pltpu.make_async_copy(at, buf.at[slot], sems.at[slot])


def norm_kernel(tile, depth, p_ref, u_ref, buf, obuf, sems, osems):
    total = p_ref.shape[0]
    steps = total // tile
    width = p_ref.shape[1] // CHUNKS
    load = lambda i, slot: fetch(p_ref, buf, sems, tile, i, slot)

    def store(i, slot):
        rows = pl.ds(pl.multiple_of(i * tile, tile), tile)
        return pltpu.make_async_copy(obuf.at[slot], u_ref.at[:, rows, :], osems.at[slot])

    for i in range(min(depth, steps)):
        load(i, i).start()
    sub = min(64, tile)

    def step(i, carry):
        slot = lax.rem(i, depth)
        load(i, slot).wait()

        @pl.when(i >= depth)
        def _():
            store(i - depth, slot).wait()

        def inner(t, c):
            rows = pl.ds(pl.multiple_of(t * sub, sub), sub)
            x = buf[slot, rows, :].astype(F32)
            y = (x * lax.rsqrt(jnp.sum(x * x, axis=1, keepdims=True) + NORM_EPS)).astype(BF16)
            for c4 in range(CHUNKS):
                obuf[slot, c4, rows, :] = y[:, c4 * width : (c4 + 1) * width]
            return c

        lax.fori_loop(0, tile // sub, inner, 0)
        store(i, slot).start()

        @pl.when(i + depth < steps)
        def _():
            load(i + depth, slot).start()

        return carry

    lax.fori_loop(0, steps, step, 0)
    for i in range(max(steps - depth, 0), steps):
        store(i, i % depth).wait()


def order(fast, core, own, sib):
    if not fast:
        return own, sib
    return jnp.where(core == 0, own, sib), jnp.where(core == 0, sib, own)


def position(fast):
    if not fast:
        return 0, 0
    me = lax.axis_index("proto")
    return lax.div(me, 2), lax.rem(me, 2)


def square(x):
    y = x.astype(F32)
    return y * y


def chunk_kernel(fast, slot, last, scale, tile, load, *refs):
    own_ref, sib_ref, unit = refs[:3]
    at = 3
    if slot:
        k_in = refs[at : at + HALVES]
        sq_in = refs[at + HALVES]
        at += HALVES + 1
    k_out = refs[at : at + HALVES]
    extra, lhs, buf, sems = refs[at + HALVES : at + HALVES + 4]
    z, core = position(fast)
    zc = lax.bitwise_xor(z, slot) if fast else slot
    half = k_out[0].shape[1]
    depth = buf.shape[0]
    steps = HALVES * half // load
    copy = lambda i, b: fetch(unit, buf, sems, load, i, b, chunk=zc)
    for i in range(min(depth, steps)):
        copy(i, i).start()
    own, sib = own_ref[...], sib_ref[...]
    first, second = order(fast, core, own, sib)
    width = own.shape[1]
    lhs[:, :width] = first
    lhs[:, width:] = second
    sq = square(own) + square(sib)
    if slot:
        sq = sq + sq_in[...]
    if not last:
        extra[...] = sq
    else:
        inv = refs[at + HALVES + 4]
        total = jnp.sum(sq, axis=1, keepdims=True)
        inv[...] = jnp.broadcast_to(lax.rsqrt(total + NORM_EPS) * scale, inv.shape)
    for h in range(HALVES):

        def step(j, carry, h=h):
            i = h * (half // load) + j
            b = lax.rem(i, depth)
            copy(i, b).wait()

            def inner(n, c):
                base = pl.multiple_of(j * load + n * tile, tile)
                d = lax.dot_general(
                    lhs[...],
                    buf[b, pl.ds(pl.multiple_of(n * tile, tile), tile), :],
                    (((1,), (1,)), ((), ())),
                    preferred_element_type=F32,
                )
                cols = pl.ds(base, tile)
                if slot:
                    d = d + k_in[h][:, cols]
                if last:
                    sums = []
                    for l in range(tile // LANES):
                        e = jnp.exp(d[:, l * LANES : (l + 1) * LANES] * inv[...])
                        k_out[h][:, pl.ds(pl.multiple_of(base + l * LANES, LANES), LANES)] = e
                        sums.append(jnp.sum(e, axis=0, keepdims=True))
                    extra[:, pl.ds(pl.multiple_of(h * half + base, tile), tile)] = jnp.concatenate(sums, axis=1)
                else:
                    k_out[h][:, cols] = d
                return c

            lax.fori_loop(0, load // tile, inner, 0)

            @pl.when(i + depth < steps)
            def _():
                copy(i + depth, b).start()

            return carry

        lax.fori_loop(0, half // load, step, 0)


def row_pass_kernel(parts, scale, group, keep, *refs):
    cs = refs[:parts]
    k = refs[parts : parts + HALVES]
    out = refs[parts + HALVES]
    at = parts + HALVES + 1
    if keep:
        c_ref = refs[at]
        at += 1
    else:
        c_ref = refs[at]
        at += 1
    acc = refs[at]
    total = cs[0][...]
    for p in cs[1:]:
        total = total + p[...]
    c_ref[...] = 1.0 / (scale * total)
    rows_all = k[0].shape[0]
    half = k[0].shape[1]
    block = 64
    acc[...] = jnp.zeros(acc.shape, F32)
    for h in range(HALVES):

        def step(g, carry, h=h):
            cvec = c_ref[:, pl.ds(pl.multiple_of(h * half + g * group, group), group)]

            def inner(t, c):
                rows = pl.ds(pl.multiple_of(t * block, block), block)
                s = acc[rows, :]
                for i in range(group // LANES):
                    cols = pl.ds(pl.multiple_of(g * group + i * LANES, LANES), LANES)
                    s = s + k[h][rows, cols] * cvec[:, i * LANES : (i + 1) * LANES]
                acc[rows, :] = s
                return c

            lax.fori_loop(0, rows_all // block, inner, 0, unroll=2)
            return carry

        lax.fori_loop(0, half // group, step, 0)
    out[...] = rows_to_lanes(acc[...])


def col_pass_kernel(parts, scale, group, *refs):
    rs = refs[:parts]
    k = refs[parts : parts + HALVES]
    out, rb = refs[parts + HALVES :]
    total = rs[0][...]
    for p in rs[1:]:
        total = total + p[...]
    lanes_to_rows(1.0 / (scale * total), rb)
    rows_all = k[0].shape[0]
    half = k[0].shape[1]
    block = 64
    count = group // LANES
    for h in range(HALVES):

        def step(g, carry, h=h):
            def inner(t, accs):
                rows = pl.ds(pl.multiple_of(t * block, block), block)
                r = rb[rows, :]
                new = []
                for i in range(count):
                    cols = pl.ds(pl.multiple_of(g * group + i * LANES, LANES), LANES)
                    x = k[h][rows, cols] * r
                    new.append(accs[i] + jnp.sum(x.reshape(block // 8, 8, LANES), axis=0))
                return tuple(new)

            accs = lax.fori_loop(
                0, rows_all // block, inner, tuple(jnp.zeros((8, LANES), F32) for _ in range(count)), unroll=2
            )
            sums = [jnp.sum(a, axis=0, keepdims=True) for a in accs]
            out[:, pl.ds(pl.multiple_of(h * half + g * group, group), group)] = jnp.concatenate(sums, axis=1)
            return carry

        lax.fori_loop(0, half // group, step, 0)


def prep_kernel(fast, scale, *refs):
    own = refs[:CHUNKS]
    sib = refs[CHUNKS : 2 * CHUNKS]
    lhs, inv = refs[2 * CHUNKS :]
    z, core = position(fast)
    width = own[0].shape[1]
    sq = jnp.zeros(inv.shape, F32)
    for s in range(CHUNKS):
        a, b = own[s][...], sib[s][...]
        first, second = order(fast, core, a, b)
        lhs[s, :, :width] = first
        lhs[s, :, width:] = second
        sq = sq + square(a) + square(b)
    total = jnp.sum(sq, axis=1, keepdims=True)
    inv[...] = jnp.broadcast_to(lax.rsqrt(total + NORM_EPS) * scale, inv.shape)


def logit_kernel(fast, offset, tile, lhs, inv, unit, tot_in, tot_out, q_ref, buf, qbuf, sems, qsems):
    z, core = position(fast)
    piece = q_ref.shape[1]
    depth = buf.shape[0]
    steps = piece // tile

    def copy(i, b):
        rows = pl.ds(pl.multiple_of(offset + i * tile, tile), tile)
        return pltpu.make_async_copy(unit.at[:, rows, :], buf.at[b], sems.at[b])

    def store(i, b):
        cols = pl.ds(pl.multiple_of(i * tile, tile), tile)
        return pltpu.make_async_copy(qbuf.at[b], q_ref.at[:, cols], qsems.at[b])

    for i in range(min(depth, steps)):
        copy(i, i).start()
    tot_out[...] = tot_in[...]

    def step(n, carry):
        b = lax.rem(n, depth)
        copy(n, b).wait()
        w = lax.rem(n, 2)

        @pl.when(n >= 2)
        def _():
            store(n - 2, w).wait()

        d = None
        for s in range(CHUNKS):
            zc = lax.bitwise_xor(z, s) if fast else s
            part = lax.dot_general(
                lhs[s], buf[b, zc], (((1,), (1,)), ((), ())), preferred_element_type=F32
            )
            d = part if d is None else d + part
        for i in range(tile // LANES):
            logit = d[:, i * LANES : (i + 1) * LANES] * inv[...]
            tot_out[...] += jnp.exp(logit)
            q = jnp.round(logit * LOGIT_STEPS).astype(jnp.int32).astype(jnp.int16)
            qbuf[w, :, i * LANES : (i + 1) * LANES] = q
        store(n, w).start()

        @pl.when(n + depth < steps)
        def _():
            copy(n + depth, b).start()

        return carry

    lax.fori_loop(0, steps, step, 0)
    for i in range(max(steps - 2, 0), steps):
        store(i, i % 2).wait()


def cross_kernel(group, *refs):
    k = refs[:HALVES]
    q = refs[HALVES : HALVES + PIECES]
    c_ref, tot, out, acc, buf, sems = refs[HALVES + PIECES :]
    depth = buf.shape[0]
    copy = lambda j: pltpu.make_async_copy(q[j], buf.at[j % depth], sems.at[j % depth])
    for j in range(depth):
        copy(j).start()
    rows_all = k[0].shape[0]
    piece = q[0].shape[1]
    per_half = PIECES // HALVES
    block = 64
    acc[...] = jnp.zeros(acc.shape, F32)
    for j in range(PIECES):
        h, base = j // per_half, (j % per_half) * piece
        copy(j).wait()

        def step(g, carry, j=j, h=h, base=base):
            cvec = c_ref[:, pl.ds(pl.multiple_of(j * piece + g * group, group), group)] * (1.0 / LOGIT_STEPS)

            def inner(t, c):
                rows = pl.ds(pl.multiple_of(t * block, block), block)
                s = acc[rows, :]
                for i in range(group // LANES):
                    qc = pl.ds(pl.multiple_of(g * group + i * LANES, LANES), LANES)
                    kc = pl.ds(pl.multiple_of(base + g * group + i * LANES, LANES), LANES)
                    lo = buf[j % depth, rows, qc].astype(jnp.int32).astype(F32)
                    s = s + (k[h][rows, kc] * cvec[:, i * LANES : (i + 1) * LANES]) * lo
                acc[rows, :] = s
                return c

            lax.fori_loop(0, rows_all // block, inner, 0)
            return carry

        lax.fori_loop(0, piece // group, step, 0)
        if j + depth < PIECES:
            copy(j + depth).start()
    blocks = rows_all // LANES
    out[:blocks, :] = rows_to_lanes(tot[...])
    out[blocks:, :] = rows_to_lanes(acc[...])


def write_kernel(parts, scale, tile, *refs):
    rs = refs[:parts]
    k = refs[parts : parts + HALVES]
    c_ref = refs[parts + HALVES]
    out, rb, buf, sems = refs[parts + HALVES + 1 :]
    total = rs[0][...]
    for p in rs[1:]:
        total = total + p[...]
    lanes_to_rows(scale / total, rb)
    rows_all = k[0].shape[0]
    half = k[0].shape[1]
    depth = buf.shape[0]
    steps = rows_all // tile

    def copy(i, slot):
        return pltpu.make_async_copy(
            buf.at[slot], out.at[pl.ds(pl.multiple_of(i * tile, tile), tile), :], sems.at[slot]
        )

    def step(i, carry):
        slot = lax.rem(i, depth)

        @pl.when(i >= depth)
        def _():
            copy(i - depth, slot).wait()

        rows = pl.ds(pl.multiple_of(i * tile, tile), tile)
        r = rb[rows, :]
        for h in range(HALVES):

            def inner(n, c, h=h):
                kc = pl.ds(pl.multiple_of(n * LANES, LANES), LANES)
                oc = pl.ds(pl.multiple_of(h * half + n * LANES, LANES), LANES)
                buf[slot, :, oc] = (k[h][rows, kc] * c_ref[:, oc] * r).astype(BF16)
                return c

            lax.fori_loop(0, half // LANES, inner, 0, unroll=4)
        copy(i, slot).start()
        return carry

    lax.fori_loop(0, steps, step, 0)
    for i in range(max(steps - depth, 0), steps):
        copy(i, i % depth).wait()


def swap(x, axis, distance):
    n = lax.axis_size(axis)
    return lax.ppermute(x, axis, [(i, i ^ distance) for i in range(n)])


def radices(n):
    out = []
    while n % 4 == 0:
        out.append(4)
        n //= 4
    if n > 1:
        out.insert(0, n)
    return out


def reduce_parts(x, axis, steps):
    stride = 1
    parts = [x]
    for radix in steps:
        if len(parts) > 1:
            x = functools.reduce(lambda a, b: a + b, parts)
        parts = [x] + [swap(x, axis, stride * d) for d in range(1, radix)]
        stride *= radix
    return parts


def slices_fast(x):
    core = lambda v: swap(v, "proto", 1)
    s0 = x
    s2 = swap(x, "proto", 4)
    s1 = swap(x, "proto", 2)
    s3 = swap(s2, "proto", 2)
    own = [s0, s1, s2, s3]
    return own, [core(v) for v in own]


def slices_plain(x, width):
    full = lax.all_gather(x, "proto", axis=1, tiled=True)
    parts = [full[:, i * width : (i + 1) * width] for i in range(2 * CHUNKS)]
    return parts[0::2], parts[1::2]


def local(view_codes, predictor_view_embeddings, prototypes):
    nb, npr = lax.axis_size("batch"), lax.axis_size("proto")
    rows = view_codes.shape[0]
    cols, dim = prototypes.shape
    half = cols // HALVES
    width = dim // CHUNKS
    piece = cols // PIECES
    rows_total, protos_total = rows * nb, cols * npr
    fast = npr == 8 and view_codes.shape[1] * 2 == width
    tile = min(256, piece)
    group = min(1024, piece)
    sds = jax.ShapeDtypeStruct
    vec = sds((1, cols), F32)
    packed = sds((rows // LANES, LANES), F32)

    ntile = min(512, half)
    load = min(1024, half)
    unit = call(
        functools.partial(norm_kernel, ntile, 4),
        pltpu.HBM((CHUNKS, cols, width), BF16),
        [HB],
        (prototypes,),
        scratch=[
            pltpu.VMEM((4, ntile, dim), BF16),
            pltpu.VMEM((4, CHUNKS, ntile, width), BF16),
            pltpu.SemaphoreType.DMA((4,)),
            pltpu.SemaphoreType.DMA((4,)),
        ],
        limit=14,
        flops=5e9,
        name="unit_rows",
    )
    gather = slices_fast if fast else functools.partial(slices_plain, width=width // 2)
    own1, sib1 = gather(view_codes)
    own2, sib2 = gather(predictor_view_embeddings)

    k = ()
    sq = ()
    kshape = tuple(pltpu.VMEM((rows, half), F32) for _ in range(HALVES))
    for s in range(CHUNKS):
        last = s == CHUNKS - 1
        nin = 3
        res = call(
            functools.partial(chunk_kernel, fast, s, last, 1.0 / EPSILON, tile, load),
            kshape + ((vec,) if last else (sds((rows, LANES), F32),)),
            [VM, VM, HB] + [VM] * (HALVES + 1 if s else 0),
            (own1[s], sib1[s], unit, *k, *sq),
            scratch=[
                pltpu.VMEM((rows, width), BF16),
                pltpu.VMEM((3, load, width), BF16),
                pltpu.SemaphoreType.DMA((3,)),
            ]
            + ([pltpu.VMEM((rows, LANES), F32)] if last else []),
            limit=8,
            alias={nin + h: h for h in range(HALVES)} if s else None,
            flops=2 * rows * cols * width,
            name=f"scores_{s}",
        )
        k, sq = res[:HALVES], res[HALVES:]
    col_part = sq[0]

    lhs2, inv2 = call(
        functools.partial(prep_kernel, fast, 1.0 / SOFTMAX_TEMP_VALUE),
        (sds((CHUNKS, rows, width), BF16), sds((rows, LANES), F32)),
        [VM] * (2 * CHUNKS),
        (*own2, *sib2),
        flops=5e8,
        name="second_view",
    )
    tot = jnp.zeros((rows, LANES), F32)
    quant = []
    for j in range(PIECES):
        tot, q = call(
            functools.partial(logit_kernel, fast, j * piece, min(tile, piece)),
            (sds((rows, LANES), F32), pltpu.HBM((rows, piece), jnp.int16)),
            [VM, VM, HB, VM],
            (lhs2, inv2, unit, tot),
            scratch=[
                pltpu.VMEM((3, CHUNKS, min(tile, piece), width), BF16),
                pltpu.VMEM((2, rows, min(tile, piece)), jnp.int16),
                pltpu.SemaphoreType.DMA((3,)),
                pltpu.SemaphoreType.DMA((2,)),
            ],
            limit=8,
            flops=2 * rows * piece * dim,
            name=f"logits_{j}",
        )
        quant.append(q)

    for it in range(SINK_ITERS):
        cparts = reduce_parts(col_part, "batch", radices(nb))
        keep = it == SINK_ITERS - 1
        res = call(
            functools.partial(row_pass_kernel, len(cparts), float(protos_total), group, keep),
            (packed, vec),
            [VM] * (len(cparts) + HALVES),
            (*cparts, *k),
            scratch=[pltpu.VMEM((rows, LANES), F32)],
            flops=4e9,
            name=f"row_pass_{it}",
        )
        row_part, c = res
        if not keep:
            rparts = reduce_parts(row_part, "proto", radices(npr))
            col_part = call(
                functools.partial(col_pass_kernel, len(rparts), float(rows_total), group),
                vec,
                [VM] * (len(rparts) + HALVES),
                (*rparts, *k),
                scratch=[pltpu.VMEM((rows, LANES), F32)],
                flops=4e9,
                name=f"col_pass_{it}",
            )

    rparts = reduce_parts(row_part, "proto", radices(npr))
    both = call(
        functools.partial(cross_kernel, min(512, piece)),
        sds((2 * (rows // LANES), LANES), F32),
        [VM] * HALVES + [HB] * PIECES + [VM] * 2,
        (*k, *quant, c, tot),
        scratch=[
            pltpu.VMEM((rows, LANES), F32),
            pltpu.VMEM((3, rows, piece), jnp.int16),
            pltpu.SemaphoreType.DMA((3,)),
        ],
        limit=10,
        flops=4e9,
        name="cross",
    )
    bparts = reduce_parts(both, "proto", radices(npr))
    otile = 64
    assignments = call(
        functools.partial(write_kernel, len(rparts), float(protos_total), otile),
        pltpu.HBM((rows, cols), BF16),
        [VM] * (len(rparts) + HALVES + 1),
        (*rparts, *k, c),
        scratch=[
            pltpu.VMEM((rows, LANES), F32),
            pltpu.VMEM((3, otile, cols), BF16),
            pltpu.SemaphoreType.DMA((3,)),
        ],
        flops=4e9,
        name="write",
    )
    add = lambda ps: functools.reduce(lambda a, b: a + b, ps)
    blocks = rows // LANES
    sums = add(bparts)
    loss = jnp.log(sums[:blocks]) - sums[blocks:] / add(rparts)
    return assignments, loss.reshape(rows)


def solution(mesh):
    placed = (P("batch", "proto"), P("batch", "proto"), P("proto", None))
    return jax.shard_map(
        local,
        mesh=mesh,
        in_specs=placed,
        out_specs=(P("batch", "proto"), P("batch")),
        check_vma=False,
    )
```

```python
import functools

import jax
import jax.numpy as jnp
from jax import lax
from jax.experimental import pallas as pl
from jax.experimental.pallas import tpu as pltpu
from jax.sharding import PartitionSpec as P

SINK_ITERS = 3
EPSILON = 0.05
SOFTMAX_TEMP_VALUE = 0.1
NORM_EPS = 1e-06
CHUNKS = 4
HALVES = 4
PIECES = 8
NEAR = 2 * CHUNKS
COVER = (2, 2, 2, 1, 1)
LANES = 128
LOG2E = 1.4426950408889634
LOGIT_STEPS = 2200.0


F32 = jnp.float32
BF16 = jnp.bfloat16
VM = pl.BlockSpec(memory_space=pltpu.VMEM)
HB = pl.BlockSpec(memory_space=pltpu.HBM)


def call(kernel, outs, ins, args, scratch=(), limit=6, flops=0, alias=None):
    big = lambda a: a.size * a.dtype.itemsize > (4 << 20)
    args = [
        pltpu.with_memory_space_constraint(a, pltpu.HBM if spec is HB else pltpu.VMEM) if spec is HB or big(a) else a
        for a, spec in zip(args, ins)
    ]
    return pl.pallas_call(
        kernel,
        out_shape=outs,
        in_specs=ins,
        out_specs=jax.tree.map(
            lambda o: HB if getattr(o, "memory_space", None) == pltpu.HBM else VM, outs
        ),
        scratch_shapes=list(scratch),
        input_output_aliases=alias or {},
        compiler_params=pltpu.CompilerParams(vmem_limit_bytes=limit << 20),
        cost_estimate=pl.CostEstimate(flops=int(flops), bytes_accessed=0, transcendentals=0),
    )(*args)


def rows_to_lanes(block):
    out = []
    for i in range(block.shape[0] // LANES):
        part = block[i * LANES : (i + 1) * LANES, :]
        out.append(jnp.sum(part.T, axis=0, keepdims=True))
    return jnp.concatenate(out, axis=0)


def lanes_to_rows(packed, out_ref):
    for i in range(packed.shape[0]):
        row = jnp.broadcast_to(packed[i : i + 1, :], (LANES, LANES))
        out_ref[i * LANES : (i + 1) * LANES, :] = row.T


def fetch(src, buf, sems, tile, i, slot):
    rows = pl.ds(pl.multiple_of(i * tile, tile), tile)
    return pltpu.make_async_copy(src.at[rows, :], buf.at[slot], sems.at[slot])


def norm_kernel(tile, depth, p_ref, u_ref, buf, obuf, inv, sems, osems):
    total = p_ref.shape[0]
    steps = total // tile
    width = p_ref.shape[1] // CHUNKS
    load = lambda i, slot: fetch(p_ref, buf, sems, tile, i, slot)

    def store(i, slot):
        rows = pl.ds(pl.multiple_of(i * tile, tile), tile)
        return pltpu.make_async_copy(obuf.at[slot], u_ref.at[:, rows, :], osems.at[slot])

    for i in range(min(depth, steps)):
        load(i, i).start()
    sub = min(32, tile)

    def step(i, carry):
        slot = lax.rem(i, depth)
        load(i, slot).wait()

        @pl.when(i >= depth)
        def _():
            store(i - depth, slot).wait()

        def sums(t, c):
            rows = pl.ds(pl.multiple_of(t * sub, sub), sub)
            x = buf[slot, rows, :].astype(F32)
            total = jnp.sum(x * x, axis=1, keepdims=True)
            inv[rows, :] = jnp.broadcast_to(lax.rsqrt(total + NORM_EPS), (sub, LANES))
            return c

        def scale(t, c):
            rows = pl.ds(pl.multiple_of(t * sub, sub), sub)
            r = inv[rows, :]
            for l in range(CHUNKS * width // LANES):
                x = buf[slot, rows, l * LANES : (l + 1) * LANES].astype(F32)
                at = l * LANES % width
                obuf[slot, l * LANES // width, rows, at : at + LANES] = (x * r).astype(BF16)
            return c

        lax.fori_loop(0, tile // sub, sums, 0, unroll=8)
        lax.fori_loop(0, tile // sub, scale, 0, unroll=2)
        store(i, slot).start()

        @pl.when(i + depth < steps)
        def _():
            load(i + depth, slot).start()

        return carry

    lax.fori_loop(0, steps, step, 0)
    for i in range(max(steps - depth, 0), steps):
        store(i, i % depth).wait()


def order(fast, core, own, sib):
    if not fast:
        return own, sib
    return jnp.where(core == 0, own, sib), jnp.where(core == 0, sib, own)


def position(fast):
    if not fast:
        return 0, 0
    me = lax.axis_index("proto")
    return lax.div(me, 2), lax.rem(me, 2)


def square(x):
    y = x.astype(F32)
    return y * y


def stage_kernel(fast, slots, last, scale, tile, block, *refs):
    count = len(slots)
    own = refs[:count]
    sib = refs[count : 2 * count]
    unit = refs[2 * count]
    at = 2 * count + 1
    if last:
        sq_in = refs[at + HALVES]
        at += HALVES + 1
    k = refs[at : at + HALVES]
    extra, lhs, inv, buf, sems, csum = refs[at + HALVES :]
    z, core = position(fast)
    half = k[0].shape[1]
    rows_all = k[0].shape[0]

    def copies(h):
        return [
            pltpu.make_async_copy(
                unit.at[lax.bitwise_xor(z, s) if fast else s, pl.ds(h * half, half), :],
                buf.at[h % 2, n],
                sems.at[h % 2, n],
            )
            for n, s in enumerate(slots)
        ]

    for h in range(2):
        for c in copies(h):
            c.start()
    for n in range(count):
        a, b = own[n][...], sib[n][...]
        first, second = order(fast, core, a, b)
        width = a.shape[1]
        lhs[n, :, :width] = first
        lhs[n, :, width:] = second
    step = min(64, rows_all)

    def squares(t, c):
        rows = pl.ds(pl.multiple_of(t * step, step), step)
        sq = sq_in[rows, :] if last else jnp.zeros((step, LANES), F32)
        for n in range(count):
            for l in range(lhs.shape[2] // LANES):
                sq = sq + square(lhs[n, rows, l * LANES : (l + 1) * LANES])
        if last:
            total = jnp.sum(sq, axis=1, keepdims=True)
            inv[rows, :] = jnp.broadcast_to(lax.rsqrt(total + NORM_EPS) * scale, (step, LANES))
        else:
            extra[rows, :] = sq
        return c

    lax.fori_loop(0, rows_all // step, squares, 0, unroll=2)
    if last:
        csum[...] = jnp.zeros(csum.shape, F32)
    for h in range(HALVES):
        for c in copies(h):
            c.wait()

        def body(t, carry, h=h):
            rows = pl.ds(pl.multiple_of(t * block, block), block)
            for n in range(half // tile):
                d = None
                for i in range(count):
                    p = lax.dot_general(
                        lhs[i, rows, :],
                        buf[h % 2, i, n * tile : (n + 1) * tile, :],
                        (((1,), (1,)), ((), ())),
                        preferred_element_type=F32,
                    )
                    d = p if d is None else d + p
                for l in range(tile // LANES):
                    cols = slice(n * tile + l * LANES, n * tile + (l + 1) * LANES)
                    x = d[:, l * LANES : (l + 1) * LANES]
                    if last:
                        x = jnp.exp2((x + k[h][rows, cols]) * inv[rows, :])
                        full = slice(h * half + cols.start, h * half + cols.stop)
                        csum[:, full] += jnp.sum(x.reshape(block // 8, 8, LANES), axis=0)
                    k[h][rows, cols] = x
            return carry

        lax.fori_loop(0, rows_all // block, body, 0)
        if h + 2 < HALVES:
            for c in copies(h + 2):
                c.start()
    if last:
        extra[...] = jnp.sum(csum[...], axis=0, keepdims=True)


def tree(terms):
    while len(terms) > 1:
        paired = [terms[i] + terms[i + 1] for i in range(0, len(terms) - 1, 2)]
        terms = paired + ([terms[-1]] if len(terms) % 2 else [])
    return terms[0]


def col_scale(cs, scale, c_ref):
    total = cs[0][...]
    for p in cs[1:]:
        total = total + p[...]
    if total.shape[0] > 1:
        total = jnp.sum(total, axis=0, keepdims=True)
    c_ref[...] = 1.0 / (scale * total)


def spread(c_ref, start, count):
    return [
        jnp.broadcast_to(c_ref[:, start + i * LANES : start + (i + 1) * LANES], (8, LANES)) for i in range(count)
    ]


def row_pass_kernel(parts, scale, *refs):
    cs = refs[:parts]
    k = refs[parts : parts + HALVES]
    out, c_ref, acc = refs[parts + HALVES :]
    col_scale(cs, scale, c_ref)
    rows_all, half = k[0].shape
    block = min(128, rows_all)
    count = half // LANES
    for h in range(HALVES):
        cb = spread(c_ref, h * half, count)

        def inner(t, carry, h=h, cb=cb):
            for u in range(block // 8):
                rows = pl.ds(pl.multiple_of(t * block + u * 8, 8), 8)
                x = k[h][rows, :]
                s = tree([x[:, i * LANES : (i + 1) * LANES] * cb[i] for i in range(count)])
                acc[rows, :] = acc[rows, :] + s if h else s
            return carry

        lax.fori_loop(0, rows_all // block, inner, 0)
    out[...] = rows_to_lanes(acc[...])


def col_pass_kernel(parts, scale, *refs):
    rs = refs[:parts]
    k = refs[parts : parts + HALVES]
    out, rb = refs[parts + HALVES :]
    total = rs[0][...]
    for p in rs[1:]:
        total = total + p[...]
    lanes_to_rows(1.0 / (scale * total), rb)
    rows_all, half = k[0].shape
    block = min(64, rows_all)
    count = half // LANES
    for h in range(HALVES):

        def inner(t, accs, h=h):
            accs = list(accs)
            for u in range(block // 8):
                rows = pl.ds(pl.multiple_of(t * block + u * 8, 8), 8)
                x = k[h][rows, :]
                r = rb[rows, :]
                for i in range(count):
                    accs[i] = accs[i] + x[:, i * LANES : (i + 1) * LANES] * r
            return tuple(accs)

        accs = lax.fori_loop(0, rows_all // block, inner, tuple(jnp.zeros((8, LANES), F32) for _ in range(count)))
        for i in range(count):
            at = h * half + i * LANES
            out[:, at : at + LANES] = jnp.sum(accs[i], axis=0, keepdims=True)


def last_pass_kernel(parts, scale, *refs):
    cs = refs[:parts]
    k = refs[parts : parts + HALVES]
    q = refs[parts + HALVES : parts + HALVES + PIECES]
    tot, out, c_ref, acc, cross, buf, sems = refs[parts + HALVES + PIECES :]
    depth = buf.shape[0]
    copy = lambda j: pltpu.make_async_copy(q[j], buf.at[j % depth], sems.at[j % depth])
    for j in range(depth):
        copy(j).start()
    col_scale(cs, scale, c_ref)
    rows_all, _ = k[0].shape
    piece = q[0].shape[1]
    per_half = PIECES // HALVES
    block = min(64, rows_all)
    count = piece // LANES
    for j in range(PIECES):
        h, base = j // per_half, (j % per_half) * piece
        cb = spread(c_ref, j * piece, count)
        copy(j).wait()

        def inner(t, carry, j=j, h=h, base=base, cb=cb):
            for u in range(block // 16):
                both = pl.ds(pl.multiple_of(t * block + u * 16, 16), 16)
                logit = buf[j % depth, both, :].astype(jnp.int32).astype(F32)
                for v in range(2):
                    rows = pl.ds(pl.multiple_of(t * block + u * 16 + v * 8, 8), 8)
                    x = k[h][rows, base : base + piece]
                    a = [x[:, i * LANES : (i + 1) * LANES] * cb[i] for i in range(count)]
                    w = [a[i] * logit[v * 8 : v * 8 + 8, i * LANES : (i + 1) * LANES] for i in range(count)]
                    s, w = tree(a), tree(w)
                    acc[rows, :] = acc[rows, :] + s if j else s
                    cross[rows, :] = cross[rows, :] + w if j else w
            return carry

        lax.fori_loop(0, rows_all // block, inner, 0)
        if j + depth < PIECES:
            copy(j + depth).start()
    blocks = rows_all // LANES
    out[:blocks, :] = rows_to_lanes(acc[...])
    out[blocks : 2 * blocks, :] = rows_to_lanes(tot[...])
    out[2 * blocks :, :] = rows_to_lanes(cross[...]) * (1.0 / (LOGIT_STEPS * LOG2E))


def piece_copies(fast, z, offset, unit, buf, sems):
    piece = buf.shape[1]
    return [
        pltpu.make_async_copy(
            unit.at[lax.bitwise_xor(z, s) if fast else s, pl.ds(offset, piece), :], buf.at[s], sems.at[s]
        )
        for s in range(CHUNKS)
    ]


def prep_kernel(fast, scale, *refs):
    own = refs[:CHUNKS]
    sib = refs[CHUNKS : 2 * CHUNKS]
    unit, lhs, inv, ahead, sems = refs[2 * CHUNKS :]
    z, core = position(fast)
    copies = piece_copies(fast, z, 0, unit, ahead, sems)
    for c in copies:
        c.start()
    width = own[0].shape[1]
    sq = jnp.zeros(inv.shape, F32)
    for s in range(CHUNKS):
        a, b = own[s][...], sib[s][...]
        first, second = order(fast, core, a, b)
        lhs[s, :, :width] = first
        lhs[s, :, width:] = second
        sq = sq + square(a) + square(b)
    total = jnp.sum(sq, axis=1, keepdims=True)
    inv[...] = jnp.broadcast_to(lax.rsqrt(total + NORM_EPS) * scale, inv.shape)
    for c in copies:
        c.wait()


def logit_kernel(fast, offset, tile, block, *refs):
    lhs, inv, buf = refs[:3]
    if offset is None:
        tot_in, tot_out, q_ref, qbuf, qsems = refs[3:]
        copies = []
    else:
        unit, tot_in, tot_out, q_ref, ahead, qbuf, qsems, sems = refs[3:]
        copies = piece_copies(fast, position(fast)[0], offset, unit, ahead, sems)
    rows_all, piece = q_ref.shape
    steps = piece // tile

    def store(t):
        rows = pl.ds(pl.multiple_of(t * block, block), block)
        return pltpu.make_async_copy(qbuf.at[rows, :], q_ref.at[rows, :], qsems.at[t])

    for c in copies:
        c.start()

    def body(t, carry):
        rows = pl.ds(pl.multiple_of(t * block, block), block)
        for n in range(steps):
            d = None
            for s in range(CHUNKS):
                part = lax.dot_general(
                    lhs[s, rows, :],
                    buf[s, n * tile : (n + 1) * tile, :],
                    (((1,), (1,)), ((), ())),
                    preferred_element_type=F32,
                )
                d = part if d is None else d + part
            sums = []
            for l in range(tile // LANES):
                logit = d[:, l * LANES : (l + 1) * LANES] * inv[rows, :]
                sums.append(jnp.exp2(logit))
                q = jnp.round(logit * LOGIT_STEPS).astype(jnp.int32).astype(jnp.int16)
                qbuf[rows, n * tile + l * LANES : n * tile + (l + 1) * LANES] = q
            before = tot_out if n else tot_in
            tot_out[rows, :] = before[rows, :] + tree(sums)
        store(t).start()
        return carry

    lax.fori_loop(0, rows_all // block, body, 0)
    for t in range(rows_all // block):
        store(t).wait()
    for c in copies:
        c.wait()


def write_kernel(parts, scale, tile, *refs):
    rs = refs[:parts]
    k = refs[parts : parts + HALVES]
    c_ref = refs[parts + HALVES]
    out, rb, buf, sems = refs[parts + HALVES + 1 :]
    blocks = rb.shape[0] // LANES
    total = rs[0][:blocks, :]
    for p in rs[1:]:
        total = total + p[:blocks, :]
    lanes_to_rows(scale / total, rb)
    rows_all = k[0].shape[0]
    half = k[0].shape[1]
    depth = buf.shape[0]
    steps = rows_all // tile

    def copy(i, slot):
        return pltpu.make_async_copy(
            buf.at[slot], out.at[pl.ds(pl.multiple_of(i * tile, tile), tile), :], sems.at[slot]
        )

    def step(i, carry):
        slot = lax.rem(i, depth)

        @pl.when(i >= depth)
        def _():
            copy(i - depth, slot).wait()

        rows = pl.ds(pl.multiple_of(i * tile, tile), tile)
        r = rb[rows, :]
        for h in range(HALVES):
            for n in range(half // LANES):
                oc = slice(h * half + n * LANES, h * half + (n + 1) * LANES)
                x = k[h][rows, n * LANES : (n + 1) * LANES]
                buf[slot, :, oc] = (x * c_ref[:, oc] * r).astype(BF16)
        copy(i, slot).start()
        return carry

    lax.fori_loop(0, steps, step, 0)
    for i in range(max(steps - depth, 0), steps):
        copy(i, i % depth).wait()


def swap(x, axis, distance):
    n = lax.axis_size(axis)
    return lax.ppermute(x, axis, [(i, i ^ distance) for i in range(n)])


def radices(n):
    out = []
    while n % 4 == 0:
        out.append(4)
        n //= 4
    if n > 1:
        out.insert(0, n)
    return out


def reduce_parts(x, axis, steps):
    stride = 1
    parts = [x]
    for radix in steps:
        if len(parts) > 1:
            x = functools.reduce(lambda a, b: a + b, parts)
        parts = [x] + [swap(x, axis, stride * d) for d in range(1, radix)]
        stride *= radix
    return parts


def first_slices(x):
    near = swap(x, "proto", 2)
    far = swap(x, "proto", 4)
    last = swap(far, "proto", 2)
    own = [x, near, far, last]
    return own, [swap(v, "proto", 1) for v in own]


def second_slices(x, gate):
    far = [swap(x, "proto", 2 * s) for s in range(1, CHUNKS)]
    *far, gate = lax.optimization_barrier((*far, gate))
    own = [x, *far]
    return own, [swap(v, "proto", 1) for v in own], gate


def slices_plain(x, width):
    full = lax.all_gather(x, "proto", axis=1, tiled=True)
    parts = [full[:, i * width : (i + 1) * width] for i in range(2 * CHUNKS)]
    return parts[0::2], parts[1::2]


def local(view_codes, predictor_view_embeddings, prototypes):
    nb, npr = lax.axis_size("batch"), lax.axis_size("proto")
    rows = view_codes.shape[0]
    cols, dim = prototypes.shape
    half = cols // HALVES
    width = dim // CHUNKS
    piece = cols // PIECES
    rows_total, protos_total = rows * nb, cols * npr
    fast = npr == NEAR and view_codes.shape[1] * 2 == width
    sds = jax.ShapeDtypeStruct
    vec = sds((1, cols), F32)
    packed = sds((rows // LANES, LANES), F32)

    ntile = min(512, half)
    unit = call(
        functools.partial(norm_kernel, ntile, 4),
        pltpu.HBM((CHUNKS, cols, width), BF16),
        [HB],
        (prototypes,),
        scratch=[
            pltpu.VMEM((4, ntile, dim), BF16),
            pltpu.VMEM((4, CHUNKS, ntile, width), BF16),
            pltpu.VMEM((ntile, LANES), F32),
            pltpu.SemaphoreType.DMA((4,)),
            pltpu.SemaphoreType.DMA((4,)),
        ],
        limit=14,
        flops=5e9,
    )
    if fast:
        own1, sib1 = first_slices(view_codes)
    else:
        own1, sib1 = slices_plain(view_codes, width // 2)

    block = min(512, rows)
    tile = min(256, piece)
    kshape = tuple(pltpu.VMEM((rows, half), F32) for _ in range(HALVES))
    k, extra = (), ()
    per_stage = CHUNKS // 2
    for s in range(2):
        last = s == 1
        slots = tuple(range(s * per_stage, (s + 1) * per_stage))
        nin = 2 * per_stage + 1
        res = call(
            functools.partial(stage_kernel, fast, slots, last, LOG2E / EPSILON, tile, block),
            kshape + (vec if last else sds((rows, LANES), F32),),
            [VM] * (nin - 1) + [HB] + [VM] * (HALVES + 1 if last else 0),
            (*[own1[i] for i in slots], *[sib1[i] for i in slots], unit, *k, *extra),
            scratch=[
                pltpu.VMEM((per_stage, rows, width), BF16),
                pltpu.VMEM((rows, LANES), F32),
                pltpu.VMEM((2, per_stage, half, width), BF16),
                pltpu.SemaphoreType.DMA((2, per_stage)),
                pltpu.VMEM((8, cols), F32),
            ],
            limit=8,
            alias={nin + h: h for h in range(HALVES)} if last else None,
            flops=2 * rows * cols * width * per_stage,
        )
        k, extra = res[:HALVES], res[HALVES:]
    col_part = extra[0]
    if fast:
        own2, sib2, col_part = second_slices(predictor_view_embeddings, col_part)
    else:
        own2, sib2 = slices_plain(predictor_view_embeddings, width // 2)

    ahead_shape = sds((CHUNKS, piece, width), BF16)
    lhs2, inv2, ahead = call(
        functools.partial(prep_kernel, fast, LOG2E / SOFTMAX_TEMP_VALUE),
        (sds((CHUNKS, rows, width), BF16), sds((rows, LANES), F32), ahead_shape),
        [VM] * (2 * CHUNKS) + [HB],
        (*own2, *sib2, unit),
        scratch=[pltpu.SemaphoreType.DMA((CHUNKS,))],
        flops=5e8,
    )
    tot = jnp.zeros((rows, LANES), F32)
    quant = []

    def logits(tot, ahead, after):
        j = len(quant)
        more = j + 1 < PIECES
        tot, after = lax.optimization_barrier((tot, after))
        tot, q, *rest = call(
            functools.partial(logit_kernel, fast, (j + 1) * piece if more else None, tile, block),
            (sds((rows, LANES), F32), pltpu.HBM((rows, piece), jnp.int16)) + ((ahead_shape,) if more else ()),
            [VM] * 3 + ([HB] if more else []) + [VM],
            (lhs2, inv2, ahead) + ((unit,) if more else ()) + (tot,),
            scratch=[pltpu.VMEM((rows, piece), jnp.int16), pltpu.SemaphoreType.DMA((rows // block,))]
            + ([pltpu.SemaphoreType.DMA((CHUNKS,))] if more else []),
            limit=6,
            flops=2 * rows * piece * dim,
        )
        quant.append(q)
        return tot, (rest[0] if more else None)

    def cover(parts, tot, ahead, count):
        for _ in range(min(count, PIECES - len(quant))):
            tot, ahead = logits(tot, ahead, parts[0])
        *head, tail = parts
        tail, tot = lax.optimization_barrier((tail, tot))
        return [*head, tail], tot, ahead

    for it in range(SINK_ITERS):
        cparts = reduce_parts(col_part, "batch", radices(nb))
        cparts, tot, ahead = cover(cparts, tot, ahead, COVER[2 * it])
        if it < SINK_ITERS - 1:
            row_part, _ = call(
                functools.partial(row_pass_kernel, len(cparts), float(protos_total)),
                (packed, vec),
                [VM] * (len(cparts) + HALVES),
                (*cparts, *k),
                scratch=[pltpu.VMEM((rows, LANES), F32)],
                flops=4e9,
            )
            rparts = reduce_parts(row_part, "proto", radices(npr))
            rparts, tot, ahead = cover(rparts, tot, ahead, COVER[2 * it + 1])
            col_part = call(
                functools.partial(col_pass_kernel, len(rparts), float(rows_total)),
                vec,
                [VM] * (len(rparts) + HALVES),
                (*rparts, *k),
                scratch=[pltpu.VMEM((rows, LANES), F32)],
                flops=4e9,
            )

    blocks = rows // LANES
    both, c = call(
        functools.partial(last_pass_kernel, len(cparts), float(protos_total)),
        (sds((3 * blocks, LANES), F32), vec),
        [VM] * (len(cparts) + HALVES) + [HB] * PIECES + [VM],
        (*cparts, *k, *quant, tot),
        scratch=[
            pltpu.VMEM((rows, LANES), F32),
            pltpu.VMEM((rows, LANES), F32),
            pltpu.VMEM((4, rows, piece), jnp.int16),
            pltpu.SemaphoreType.DMA((4,)),
        ],
        limit=12,
        flops=8e9,
    )
    bparts = reduce_parts(both, "proto", radices(npr))
    otile = 64
    assignments = call(
        functools.partial(write_kernel, len(bparts), float(protos_total), otile),
        pltpu.HBM((rows, cols), BF16),
        [VM] * (len(bparts) + HALVES + 1),
        (*bparts, *k, c),
        scratch=[
            pltpu.VMEM((rows, LANES), F32),
            pltpu.VMEM((3, otile, cols), BF16),
            pltpu.SemaphoreType.DMA((3,)),
        ],
        flops=4e9,
    )
    sums = functools.reduce(lambda a, b: a + b, bparts)
    loss = jnp.log(sums[blocks : 2 * blocks]) - sums[2 * blocks :] / sums[:blocks]
    return assignments, loss.reshape(rows)


def solution(mesh):
    placed = (P("batch", "proto"), P("batch", "proto"), P("proto", None))

    return jax.shard_map(
        local,
        mesh=mesh,
        in_specs=placed,
        out_specs=(P("batch", "proto"), P("batch")),
        check_vma=False,
    )
```

```python
import functools

import jax
import jax.numpy as jnp
from jax import lax
from jax.experimental import pallas as pl
from jax.experimental.pallas import tpu as pltpu
from jax.sharding import PartitionSpec as P

SINK_ITERS = 3
EPSILON = 0.05
SOFTMAX_TEMP_VALUE = 0.1
NORM_EPS = 1e-06
CHUNKS = 4
HALVES = 4
PIECES = 8
NEAR = 2 * CHUNKS
COVER = (2, 2, 2, 1, 1)
LANES = 128
LOG2E = 1.4426950408889634
LOGIT_STEPS = 2200.0


F32 = jnp.float32
BF16 = jnp.bfloat16
VM = pl.BlockSpec(memory_space=pltpu.VMEM)
HB = pl.BlockSpec(memory_space=pltpu.HBM)


def call(kernel, outs, ins, args, scratch=(), limit=6, flops=0, alias=None):
    big = lambda a: a.size * a.dtype.itemsize > (4 << 20)
    args = [
        pltpu.with_memory_space_constraint(a, pltpu.HBM if spec is HB else pltpu.VMEM) if spec is HB or big(a) else a
        for a, spec in zip(args, ins)
    ]
    return pl.pallas_call(
        kernel,
        out_shape=outs,
        in_specs=ins,
        out_specs=jax.tree.map(
            lambda o: HB if getattr(o, "memory_space", None) == pltpu.HBM else VM, outs
        ),
        scratch_shapes=list(scratch),
        input_output_aliases=alias or {},
        compiler_params=pltpu.CompilerParams(vmem_limit_bytes=limit << 20),
        cost_estimate=pl.CostEstimate(flops=int(flops), bytes_accessed=0, transcendentals=0),
    )(*args)


def rows_to_lanes(block):
    out = []
    for i in range(block.shape[0] // LANES):
        part = block[i * LANES : (i + 1) * LANES, :]
        out.append(jnp.sum(part.T, axis=0, keepdims=True))
    return jnp.concatenate(out, axis=0)


def lanes_to_rows(packed, out_ref):
    for i in range(packed.shape[0]):
        row = jnp.broadcast_to(packed[i : i + 1, :], (LANES, LANES))
        out_ref[i * LANES : (i + 1) * LANES, :] = row.T


def fetch(src, buf, sems, tile, i, slot):
    rows = pl.ds(pl.multiple_of(i * tile, tile), tile)
    return pltpu.make_async_copy(src.at[rows, :], buf.at[slot], sems.at[slot])


def position(fast):
    if not fast:
        return 0, 0
    me = lax.axis_index("proto")
    return lax.div(me, 2), lax.rem(me, 2)


def unit_copies(fast, slots, start, unit, buf, sems):
    z = position(fast)[0]
    count = buf.shape[1]
    return [
        pltpu.make_async_copy(
            unit.at[lax.bitwise_xor(z, s) if fast else s, pl.ds(start, count), :], buf.at[n], sems.at[n]
        )
        for n, s in enumerate(slots)
    ]


def norm_kernel(fast, slots, tile, depth, p_ref, u_ref, ahead, buf, obuf, inv, sems, osems, asems):
    total = p_ref.shape[0]
    steps = total // tile
    width = p_ref.shape[1] // CHUNKS
    load = lambda i, slot: fetch(p_ref, buf, sems, tile, i, slot)

    def store(i, slot):
        rows = pl.ds(pl.multiple_of(i * tile, tile), tile)
        return pltpu.make_async_copy(obuf.at[slot], u_ref.at[:, rows, :], osems.at[slot])

    for i in range(min(depth, steps)):
        load(i, i).start()
    sub = min(32, tile)

    def step(i, carry):
        slot = lax.rem(i, depth)
        load(i, slot).wait()

        @pl.when(i >= depth)
        def _():
            store(i - depth, slot).wait()

        def sums(t, c):
            rows = pl.ds(pl.multiple_of(t * sub, sub), sub)
            x = buf[slot, rows, :].astype(F32)
            total = jnp.sum(x * x, axis=1, keepdims=True)
            inv[rows, :] = jnp.broadcast_to(lax.rsqrt(total + NORM_EPS), (sub, LANES))
            return c

        def scale(t, c):
            rows = pl.ds(pl.multiple_of(t * sub, sub), sub)
            r = inv[rows, :]
            for l in range(CHUNKS * width // LANES):
                x = buf[slot, rows, l * LANES : (l + 1) * LANES].astype(F32)
                at = l * LANES % width
                obuf[slot, l * LANES // width, rows, at : at + LANES] = (x * r).astype(BF16)
            return c

        lax.fori_loop(0, tile // sub, sums, 0, unroll=8)
        lax.fori_loop(0, tile // sub, scale, 0, unroll=2)
        store(i, slot).start()

        @pl.when(i + depth < steps)
        def _():
            load(i + depth, slot).start()

        return carry

    lax.fori_loop(0, steps, step, 0)
    copies = unit_copies(fast, slots, 0, u_ref, ahead, asems)
    early = steps - depth >= -(-ahead.shape[1] // tile)
    if early:
        for c in copies:
            c.start()
    for i in range(max(steps - depth, 0), steps):
        store(i, i % depth).wait()
    for c in copies:
        if not early:
            c.start()
        c.wait()


def order(fast, core, own, sib):
    if not fast:
        return own, sib
    return jnp.where(core == 0, own, sib), jnp.where(core == 0, sib, own)


def square(x):
    y = x.astype(F32)
    return y * y


def stage_kernel(fast, slots, follow, last, scale, tile, block, *refs):
    count = len(slots)
    own = refs[:count]
    sib = refs[count : 2 * count]
    unit, head = refs[2 * count : 2 * count + 2]
    at = 2 * count + 2
    if last:
        sq_in = refs[at + HALVES]
        at += HALVES + 1
    k = refs[at : at + HALVES]
    extra, ahead, lhs, inv, buf, sems, asems, csum = refs[at + HALVES :]
    _, core = position(fast)
    half = k[0].shape[1]
    rows_all = k[0].shape[0]

    def copies(h):
        return unit_copies(fast, slots, h * half, unit, buf.at[h % 2], sems.at[h % 2])

    coming = unit_copies(fast, follow, 0, unit, ahead, asems)
    for c in copies(1):
        c.start()
    for n in range(count):
        a, b = own[n][...], sib[n][...]
        first, second = order(fast, core, a, b)
        width = a.shape[1]
        lhs[n, :, :width] = first
        lhs[n, :, width:] = second
    step = min(64, rows_all)

    def squares(t, c):
        rows = pl.ds(pl.multiple_of(t * step, step), step)
        sq = sq_in[rows, :] if last else jnp.zeros((step, LANES), F32)
        for n in range(count):
            for l in range(lhs.shape[2] // LANES):
                sq = sq + square(lhs[n, rows, l * LANES : (l + 1) * LANES])
        if last:
            total = jnp.sum(sq, axis=1, keepdims=True)
            inv[rows, :] = jnp.broadcast_to(lax.rsqrt(total + NORM_EPS) * scale, (step, LANES))
        else:
            extra[rows, :] = sq
        return c

    lax.fori_loop(0, rows_all // step, squares, 0, unroll=2)
    if last:
        csum[...] = jnp.zeros(csum.shape, F32)
    for h in range(HALVES):
        if h:
            for c in copies(h):
                c.wait()
        if h + 1 == HALVES:
            for c in coming:
                c.start()
        weights = buf.at[h % 2] if h else head

        def body(t, carry, h=h, weights=weights):
            rows = pl.ds(pl.multiple_of(t * block, block), block)
            for n in range(half // tile):
                d = None
                for i in range(count):
                    p = lax.dot_general(
                        lhs[i, rows, :],
                        weights[i, n * tile : (n + 1) * tile, :],
                        (((1,), (1,)), ((), ())),
                        preferred_element_type=F32,
                    )
                    d = p if d is None else d + p
                for l in range(tile // LANES):
                    cols = slice(n * tile + l * LANES, n * tile + (l + 1) * LANES)
                    x = d[:, l * LANES : (l + 1) * LANES]
                    if last:
                        x = jnp.exp2((x + k[h][rows, cols]) * inv[rows, :])
                        full = slice(h * half + cols.start, h * half + cols.stop)
                        csum[:, full] += jnp.sum(x.reshape(block // 8, 8, LANES), axis=0)
                    k[h][rows, cols] = x
            return carry

        lax.fori_loop(0, rows_all // block, body, 0)
        if h + 2 < HALVES:
            for c in copies(h + 2):
                c.start()
    for c in coming:
        c.wait()
    if last:
        extra[...] = jnp.sum(csum[...], axis=0, keepdims=True)


def tree(terms):
    while len(terms) > 1:
        paired = [terms[i] + terms[i + 1] for i in range(0, len(terms) - 1, 2)]
        terms = paired + ([terms[-1]] if len(terms) % 2 else [])
    return terms[0]


def col_scale(cs, scale, c_ref):
    total = cs[0][...]
    for p in cs[1:]:
        total = total + p[...]
    if total.shape[0] > 1:
        total = jnp.sum(total, axis=0, keepdims=True)
    c_ref[...] = 1.0 / (scale * total)


def spread(c_ref, start, count):
    return [
        jnp.broadcast_to(c_ref[:, start + i * LANES : start + (i + 1) * LANES], (8, LANES)) for i in range(count)
    ]


def row_pass_kernel(parts, scale, *refs):
    cs = refs[:parts]
    k = refs[parts : parts + HALVES]
    out, c_ref, acc = refs[parts + HALVES :]
    col_scale(cs, scale, c_ref)
    rows_all, half = k[0].shape
    block = min(128, rows_all)
    count = half // LANES
    for h in range(HALVES):
        cb = spread(c_ref, h * half, count)

        def inner(t, carry, h=h, cb=cb):
            for u in range(block // 8):
                rows = pl.ds(pl.multiple_of(t * block + u * 8, 8), 8)
                x = k[h][rows, :]
                s = tree([x[:, i * LANES : (i + 1) * LANES] * cb[i] for i in range(count)])
                acc[rows, :] = acc[rows, :] + s if h else s
            return carry

        lax.fori_loop(0, rows_all // block, inner, 0)
    out[...] = rows_to_lanes(acc[...])


def col_pass_kernel(parts, scale, *refs):
    rs = refs[:parts]
    k = refs[parts : parts + HALVES]
    out, rb = refs[parts + HALVES :]
    total = rs[0][...]
    for p in rs[1:]:
        total = total + p[...]
    lanes_to_rows(1.0 / (scale * total), rb)
    rows_all, half = k[0].shape
    block = min(64, rows_all)
    count = half // LANES
    for h in range(HALVES):

        def inner(t, accs, h=h):
            accs = list(accs)
            for u in range(block // 8):
                rows = pl.ds(pl.multiple_of(t * block + u * 8, 8), 8)
                x = k[h][rows, :]
                r = rb[rows, :]
                for i in range(count):
                    accs[i] = accs[i] + x[:, i * LANES : (i + 1) * LANES] * r
            return tuple(accs)

        accs = lax.fori_loop(0, rows_all // block, inner, tuple(jnp.zeros((8, LANES), F32) for _ in range(count)))
        for i in range(count):
            at = h * half + i * LANES
            out[:, at : at + LANES] = jnp.sum(accs[i], axis=0, keepdims=True)


def last_pass_kernel(parts, scale, *refs):
    cs = refs[:parts]
    k = refs[parts : parts + HALVES]
    q = refs[parts + HALVES : parts + HALVES + PIECES]
    tot, out, c_ref, acc, cross, buf, sems = refs[parts + HALVES + PIECES :]
    depth = buf.shape[0]
    copy = lambda j: pltpu.make_async_copy(q[j], buf.at[j % depth], sems.at[j % depth])
    for j in range(depth):
        copy(j).start()
    col_scale(cs, scale, c_ref)
    rows_all, _ = k[0].shape
    piece = q[0].shape[1]
    per_half = PIECES // HALVES
    block = min(64, rows_all)
    count = piece // LANES
    for j in range(PIECES):
        h, base = j // per_half, (j % per_half) * piece
        cb = spread(c_ref, j * piece, count)
        copy(j).wait()

        def inner(t, carry, j=j, h=h, base=base, cb=cb):
            for u in range(block // 16):
                both = pl.ds(pl.multiple_of(t * block + u * 16, 16), 16)
                logit = buf[j % depth, both, :].astype(jnp.int32).astype(F32)
                for v in range(2):
                    rows = pl.ds(pl.multiple_of(t * block + u * 16 + v * 8, 8), 8)
                    x = k[h][rows, base : base + piece]
                    a = [x[:, i * LANES : (i + 1) * LANES] * cb[i] for i in range(count)]
                    w = [a[i] * logit[v * 8 : v * 8 + 8, i * LANES : (i + 1) * LANES] for i in range(count)]
                    s, w = tree(a), tree(w)
                    acc[rows, :] = acc[rows, :] + s if j else s
                    cross[rows, :] = cross[rows, :] + w if j else w
            return carry

        lax.fori_loop(0, rows_all // block, inner, 0)
        if j + depth < PIECES:
            copy(j + depth).start()
    blocks = rows_all // LANES
    out[:blocks, :] = rows_to_lanes(acc[...])
    out[blocks : 2 * blocks, :] = rows_to_lanes(tot[...])
    out[2 * blocks :, :] = rows_to_lanes(cross[...]) * (1.0 / (LOGIT_STEPS * LOG2E))


def prep_kernel(fast, scale, *refs):
    own = refs[:CHUNKS]
    sib = refs[CHUNKS : 2 * CHUNKS]
    lhs, inv = refs[2 * CHUNKS :]
    _, core = position(fast)
    width = own[0].shape[1]
    sq = jnp.zeros(inv.shape, F32)
    for s in range(CHUNKS):
        a, b = own[s][...], sib[s][...]
        first, second = order(fast, core, a, b)
        lhs[s, :, :width] = first
        lhs[s, :, width:] = second
        sq = sq + square(a) + square(b)
    total = jnp.sum(sq, axis=1, keepdims=True)
    inv[...] = jnp.broadcast_to(lax.rsqrt(total + NORM_EPS) * scale, inv.shape)


def logit_kernel(fast, offset, tile, block, *refs):
    lhs, inv, buf = refs[:3]
    if offset is None:
        tot_in, tot_out, q_ref, qbuf, qsems = refs[3:]
        copies = []
    else:
        unit, tot_in, tot_out, q_ref, ahead, qbuf, qsems, sems = refs[3:]
        copies = unit_copies(fast, range(CHUNKS), offset, unit, ahead, sems)
    rows_all, piece = q_ref.shape
    steps = piece // tile

    def store(t):
        rows = pl.ds(pl.multiple_of(t * block, block), block)
        return pltpu.make_async_copy(qbuf.at[rows, :], q_ref.at[rows, :], qsems.at[t])

    for c in copies:
        c.start()

    def body(t, carry):
        rows = pl.ds(pl.multiple_of(t * block, block), block)
        for n in range(steps):
            d = None
            for s in range(CHUNKS):
                part = lax.dot_general(
                    lhs[s, rows, :],
                    buf[s, n * tile : (n + 1) * tile, :],
                    (((1,), (1,)), ((), ())),
                    preferred_element_type=F32,
                )
                d = part if d is None else d + part
            sums = []
            for l in range(tile // LANES):
                logit = d[:, l * LANES : (l + 1) * LANES] * inv[rows, :]
                sums.append(jnp.exp2(logit))
                q = jnp.round(logit * LOGIT_STEPS).astype(jnp.int32).astype(jnp.int16)
                qbuf[rows, n * tile + l * LANES : n * tile + (l + 1) * LANES] = q
            before = tot_out if n else tot_in
            tot_out[rows, :] = before[rows, :] + tree(sums)
        store(t).start()
        return carry

    lax.fori_loop(0, rows_all // block, body, 0)
    for t in range(rows_all // block):
        store(t).wait()
    for c in copies:
        c.wait()


def write_kernel(parts, scale, tile, *refs):
    rs = refs[:parts]
    k = refs[parts : parts + HALVES]
    c_ref = refs[parts + HALVES]
    out, rb, buf, sems = refs[parts + HALVES + 1 :]
    blocks = rb.shape[0] // LANES
    total = rs[0][:blocks, :]
    for p in rs[1:]:
        total = total + p[:blocks, :]
    lanes_to_rows(scale / total, rb)
    rows_all = k[0].shape[0]
    half = k[0].shape[1]
    depth = buf.shape[0]
    steps = rows_all // tile

    def copy(i, slot):
        return pltpu.make_async_copy(
            buf.at[slot], out.at[pl.ds(pl.multiple_of(i * tile, tile), tile), :], sems.at[slot]
        )

    def step(i, carry):
        slot = lax.rem(i, depth)

        @pl.when(i >= depth)
        def _():
            copy(i - depth, slot).wait()

        for u in range(tile // 16):
            rows = pl.ds(pl.multiple_of(i * tile + u * 16, 16), 16)
            r = rb[rows, :]
            for h in range(HALVES):
                for n in range(half // LANES):
                    oc = slice(h * half + n * LANES, h * half + (n + 1) * LANES)
                    x = k[h][rows, n * LANES : (n + 1) * LANES]
                    buf[slot, u * 16 : u * 16 + 16, oc] = (x * c_ref[:, oc] * r).astype(BF16)
        copy(i, slot).start()
        return carry

    lax.fori_loop(0, steps, step, 0)
    for i in range(max(steps - depth, 0), steps):
        copy(i, i % depth).wait()


def swap(x, axis, distance):
    n = lax.axis_size(axis)
    return lax.ppermute(x, axis, [(i, i ^ distance) for i in range(n)])


def radices(n):
    out = []
    while n % 4 == 0:
        out.append(4)
        n //= 4
    if n > 1:
        out.insert(0, n)
    return out


def reduce_parts(x, axis, steps):
    stride = 1
    parts = [x]
    for radix in steps:
        if len(parts) > 1:
            x = functools.reduce(lambda a, b: a + b, parts)
        parts = [x] + [swap(x, axis, stride * d) for d in range(1, radix)]
        stride *= radix
    return parts


def first_slices(x):
    near = swap(x, "proto", 2)
    far = swap(x, "proto", 4)
    last = swap(far, "proto", 2)
    own = [x, near, far, last]
    return own, [swap(v, "proto", 1) for v in own]


def second_slices(x, gate):
    far = [swap(x, "proto", 2 * s) for s in range(1, CHUNKS)]
    *far, gate = lax.optimization_barrier((*far, gate))
    own = [x, *far]
    return own, [swap(v, "proto", 1) for v in own], gate


def slices_plain(x, width):
    full = lax.all_gather(x, "proto", axis=1, tiled=True)
    parts = [full[:, i * width : (i + 1) * width] for i in range(2 * CHUNKS)]
    return parts[0::2], parts[1::2]


def local(view_codes, predictor_view_embeddings, prototypes):
    nb, npr = lax.axis_size("batch"), lax.axis_size("proto")
    rows = view_codes.shape[0]
    cols, dim = prototypes.shape
    half = cols // HALVES
    width = dim // CHUNKS
    piece = cols // PIECES
    rows_total, protos_total = rows * nb, cols * npr
    fast = npr == NEAR and view_codes.shape[1] * 2 == width
    sds = jax.ShapeDtypeStruct
    vec = sds((1, cols), F32)
    packed = sds((rows // LANES, LANES), F32)

    ntile = min(512, half)
    per_stage = CHUNKS // 2
    slots = [tuple(range(s * per_stage, (s + 1) * per_stage)) for s in range(2)] + [tuple(range(CHUNKS))]
    stage_shape = sds((per_stage, half, width), BF16)
    ahead_shape = sds((CHUNKS, piece, width), BF16)
    unit, ahead = call(
        functools.partial(norm_kernel, fast, slots[0], ntile, 4),
        (pltpu.HBM((CHUNKS, cols, width), BF16), stage_shape),
        [HB],
        (prototypes,),
        scratch=[
            pltpu.VMEM((4, ntile, dim), BF16),
            pltpu.VMEM((4, CHUNKS, ntile, width), BF16),
            pltpu.VMEM((ntile, LANES), F32),
            pltpu.SemaphoreType.DMA((4,)),
            pltpu.SemaphoreType.DMA((4,)),
            pltpu.SemaphoreType.DMA((per_stage,)),
        ],
        limit=14,
        flops=5e9,
    )
    if fast:
        own1, sib1 = first_slices(view_codes)
    else:
        own1, sib1 = slices_plain(view_codes, width // 2)

    block = min(512, rows)
    tile = min(256, piece)
    kshape = tuple(pltpu.VMEM((rows, half), F32) for _ in range(HALVES))
    k, extra = (), ()
    for s in range(2):
        last = s == 1
        nin = 2 * per_stage + 2
        *res, ahead = call(
            functools.partial(stage_kernel, fast, slots[s], slots[s + 1], last, LOG2E / EPSILON, tile, block),
            kshape + (vec if last else sds((rows, LANES), F32), ahead_shape if last else stage_shape),
            [VM] * (nin - 2) + [HB, VM] + [VM] * (HALVES + 1 if last else 0),
            (*[own1[i] for i in slots[s]], *[sib1[i] for i in slots[s]], unit, ahead, *k, *extra),
            scratch=[
                pltpu.VMEM((per_stage, rows, width), BF16),
                pltpu.VMEM((rows, LANES), F32),
                pltpu.VMEM((2, per_stage, half, width), BF16),
                pltpu.SemaphoreType.DMA((2, per_stage)),
                pltpu.SemaphoreType.DMA((CHUNKS if last else per_stage,)),
                pltpu.VMEM((8, cols), F32),
            ],
            limit=8,
            alias={nin + h: h for h in range(HALVES)} if last else None,
            flops=2 * rows * cols * width * per_stage,
        )
        k, extra = res[:HALVES], res[HALVES:]
    col_part = extra[0]
    if fast:
        own2, sib2, col_part = second_slices(predictor_view_embeddings, col_part)
    else:
        own2, sib2 = slices_plain(predictor_view_embeddings, width // 2)

    lhs2, inv2 = call(
        functools.partial(prep_kernel, fast, LOG2E / SOFTMAX_TEMP_VALUE),
        (sds((CHUNKS, rows, width), BF16), sds((rows, LANES), F32)),
        [VM] * (2 * CHUNKS),
        (*own2, *sib2),
        flops=5e8,
    )
    tot = jnp.zeros((rows, LANES), F32)
    quant = []

    def logits(tot, ahead, after):
        j = len(quant)
        more = j + 1 < PIECES
        tot, after = lax.optimization_barrier((tot, after))
        tot, q, *rest = call(
            functools.partial(logit_kernel, fast, (j + 1) * piece if more else None, tile, block),
            (sds((rows, LANES), F32), pltpu.HBM((rows, piece), jnp.int16)) + ((ahead_shape,) if more else ()),
            [VM] * 3 + ([HB] if more else []) + [VM],
            (lhs2, inv2, ahead) + ((unit,) if more else ()) + (tot,),
            scratch=[pltpu.VMEM((rows, piece), jnp.int16), pltpu.SemaphoreType.DMA((rows // block,))]
            + ([pltpu.SemaphoreType.DMA((CHUNKS,))] if more else []),
            limit=6,
            flops=2 * rows * piece * dim,
        )
        quant.append(q)
        return tot, (rest[0] if more else None)

    def cover(parts, tot, ahead, count):
        for _ in range(min(count, PIECES - len(quant))):
            tot, ahead = logits(tot, ahead, parts[0])
        *head, tail = parts
        tail, tot = lax.optimization_barrier((tail, tot))
        return [*head, tail], tot, ahead

    for it in range(SINK_ITERS):
        cparts = reduce_parts(col_part, "batch", radices(nb))
        cparts, tot, ahead = cover(cparts, tot, ahead, COVER[2 * it])
        if it < SINK_ITERS - 1:
            row_part, _ = call(
                functools.partial(row_pass_kernel, len(cparts), float(protos_total)),
                (packed, vec),
                [VM] * (len(cparts) + HALVES),
                (*cparts, *k),
                scratch=[pltpu.VMEM((rows, LANES), F32)],
                flops=4e9,
            )
            rparts = reduce_parts(row_part, "proto", radices(npr))
            rparts, tot, ahead = cover(rparts, tot, ahead, COVER[2 * it + 1])
            col_part = call(
                functools.partial(col_pass_kernel, len(rparts), float(rows_total)),
                vec,
                [VM] * (len(rparts) + HALVES),
                (*rparts, *k),
                scratch=[pltpu.VMEM((rows, LANES), F32)],
                flops=4e9,
            )

    blocks = rows // LANES
    both, c = call(
        functools.partial(last_pass_kernel, len(cparts), float(protos_total)),
        (sds((3 * blocks, LANES), F32), vec),
        [VM] * (len(cparts) + HALVES) + [HB] * PIECES + [VM],
        (*cparts, *k, *quant, tot),
        scratch=[
            pltpu.VMEM((rows, LANES), F32),
            pltpu.VMEM((rows, LANES), F32),
            pltpu.VMEM((4, rows, piece), jnp.int16),
            pltpu.SemaphoreType.DMA((4,)),
        ],
        limit=12,
        flops=8e9,
    )
    bparts = reduce_parts(both, "proto", radices(npr))
    otile = 64
    assignments = call(
        functools.partial(write_kernel, len(bparts), float(protos_total), otile),
        pltpu.HBM((rows, cols), BF16),
        [VM] * (len(bparts) + HALVES + 1),
        (*bparts, *k, c),
        scratch=[
            pltpu.VMEM((rows, LANES), F32),
            pltpu.VMEM((3, otile, cols), BF16),
            pltpu.SemaphoreType.DMA((3,)),
        ],
        flops=4e9,
    )
    sums = functools.reduce(lambda a, b: a + b, bparts)
    loss = jnp.log(sums[blocks : 2 * blocks]) - sums[2 * blocks :] / sums[:blocks]
    return assignments, loss.reshape(rows)


def solution(mesh):
    placed = (P("batch", "proto"), P("batch", "proto"), P("proto", None))

    return jax.shard_map(
        local,
        mesh=mesh,
        in_specs=placed,
        out_specs=(P("batch", "proto"), P("batch")),
        check_vma=False,
    )
```
